32 devices in a mesh: row: 4 (over z), col: 8 (over y, x, core).
Axes of the slice: x: 2, y: 2, z: 4, core: 2. Of those that a mesh axis runs over, the one named last changes fastest.
Arguments:
- features: bfloat16 [64, 131072], P(None, ('row', 'col')), may hold values from -6 to 6
- tile_rows: int32 [4, 8, 512], P('row', 'col'), may hold values from 0 to 255, as said below
- tile_cols: int32 [4, 8, 512], P('row', 'col'), may hold values from 0 to 127
- tile_count: int32 [4, 8], P('row', 'col'), may hold values from 1 to 512, as said below
- tile_data: bfloat16 [4, 8, 512, 128, 128], P('row', 'col'), may hold values from -0.21875 to 0.21875
Outputs:
- filtered: bfloat16 [512, 131072], P(None, ('row', 'col'))
The draws below stay inside these ranges and needn't reach their ends.
Inputs may be any that keep to these rules, and one draw needn't show every extreme that they name: Within one device the pairs (tile_rows, tile_cols) of all 512 slots are distinct. `tile_count`: some device has all 512 slots live in every draw.
All inputs are finite; a program needn't handle non-finite values.
Results may differ from the reference program's by a relative error of at most 0.009.
Values may be sent and summed in bfloat16 or wider, within the bound.
A program may use at most 128 MiB of HBM per device.

```python
import jax
import jax.numpy as jnp
from jax import lax

CHANNELS = 64
SCALES = 8
TILE_SIZE = 128
NODES_DEV = 4096
TILES_MAX = 512
NODES = 131072
BLOCK_ROWS = 256
N_ROW = 4
N_COL = 8


def tile_cells(key):
    row_blocks = NODES_DEV * N_COL // TILE_SIZE
    col_blocks = NODES_DEV * N_ROW // TILE_SIZE
    keys = jax.random.split(jax.random.fold_in(key, 11), N_ROW * N_COL)

    def one_device(device_key):
        return jax.random.permutation(device_key, row_blocks * col_blocks)[:TILES_MAX]
    cells = jax.vmap(one_device)(keys)
    return (cells.reshape(N_ROW, N_COL, TILES_MAX).astype(jnp.int32), col_blocks)


def draw_tile_rows(key, part):
    cells, col_blocks = tile_cells(key)
    return (cells // col_blocks).astype(jnp.int32)


def draw_tile_cols(key, part):
    cells, col_blocks = tile_cells(key)
    return (cells % col_blocks).astype(jnp.int32)


def draw_tile_count(key, part):
    device_count = N_ROW * N_COL
    base_key = jax.random.fold_in(key, 23)
    full_key = jax.random.fold_in(key, 29)
    lowest = max(1, TILES_MAX // 8)
    highest = max(lowest + 1, TILES_MAX // 2 + 1)
    counts = jax.random.randint(base_key, (device_count,), lowest, highest).astype(jnp.int32)
    chosen = jax.random.permutation(full_key, device_count)[:max(1, device_count // 16)]
    counts = counts.at[chosen].set(TILES_MAX)
    return counts.reshape(N_ROW, N_COL).astype(jnp.int32)


def levels(key, shape, pieces, least, top_value):
    loudness, own = 1.0, jax.random.fold_in(key, 6)
    for axis_at, shards_of in pieces:
        draws = jnp.exp(jax.random.uniform(jax.random.fold_in(own, axis_at), (shards_of,), jnp.float32, least / len(pieces), top_value / len(pieces)))
        loudness = loudness * jnp.repeat(draws, shape[axis_at] // shards_of).reshape([-1 if axis == axis_at else 1 for axis in range(len(shape))])
    return loudness


def centred(stream_key, shape, deviation, bound, shards=(), kind=jnp.bfloat16):
    array = jax.random.normal(stream_key, shape, jnp.float32) * deviation
    if len(shards) > 0:
        array = levels(stream_key, shape, shards, -0.22, 0.18) * array
    return jnp.clip(array, min=-bound, max=bound).astype(kind)


def setup_inputs(seed: int = 0) -> dict:
    arg_keys = jax.random.split(jax.random.key(seed), 6)
    return {
        "features": centred(arg_keys[0], (CHANNELS, NODES), 1.0, 6.0, ((1, 32),)),
        "tile_rows": draw_tile_rows(jax.random.fold_in(arg_keys[5], 71), 0),
        "tile_cols": draw_tile_cols(jax.random.fold_in(arg_keys[5], 71), 0),
        "tile_count": draw_tile_count(jax.random.fold_in(arg_keys[5], 71), 0),
        "tile_data": centred(arg_keys[4], (N_ROW, N_COL, TILES_MAX, TILE_SIZE, TILE_SIZE), 768 ** -0.5, 0.21875, ((0, 4), (1, 8))),
    }


def bessel_pair(times):
    halved = times / 2.0
    square = halved * halved
    term_zero = jnp.ones_like(times)
    term_one = halved
    sum_zero = term_zero
    sum_one = term_one
    for degree in range(1, 24):
        term_zero = term_zero * square / float(degree * degree)
        term_one = term_one * square / float(degree * (degree + 1))
        sum_zero = sum_zero + term_zero
        sum_one = sum_one + term_one
    damping = jnp.exp(-times)
    return damping * sum_zero, damping * sum_one


def coefficients():
    times = 0.25 * 2.0 ** (jnp.arange(SCALES).astype(jnp.float32) / 2.0)
    bessel_zero, bessel_one = bessel_pair(times)
    return bessel_zero, -2.0 * bessel_one, 2.0 * (bessel_zero - 2.0 * bessel_one / times)


def apply_operator(field, tile_rows, tile_cols, tile_count, tile_data):
    per_block = NODES_DEV // TILE_SIZE
    blocks = field.reshape(CHANNELS, NODES // TILE_SIZE, TILE_SIZE)
    device_count = N_ROW * N_COL
    slot_rows = tile_rows.reshape(device_count, TILES_MAX)
    slot_cols = tile_cols.reshape(device_count, TILES_MAX)
    slot_live = tile_count.reshape(device_count)
    slot_data = tile_data.reshape(device_count, TILES_MAX, TILE_SIZE, TILE_SIZE)

    def one_device(summed, inputs):
        row_ids, col_ids, live_count, entries, device = inputs
        row_group = device // N_COL
        col_group = device % N_COL
        global_cols = ((col_ids // per_block) * N_COL + col_group) * per_block + col_ids % per_block
        picked = jnp.take(blocks, global_cols.astype(jnp.int32), axis=1)
        product = jnp.einsum("fgk,grk->fgr", picked.astype(jnp.float32), entries.astype(jnp.float32))
        live = (jnp.arange(TILES_MAX) < live_count).astype(jnp.float32)
        product = product * live[None, :, None]
        partial_value = jnp.zeros((CHANNELS, BLOCK_ROWS, TILE_SIZE), jnp.float32).at[:, row_ids].add(product)
        partial_value = partial_value.astype(jnp.bfloat16).astype(jnp.float32)
        offset = (row_group * BLOCK_ROWS).astype(jnp.int32)
        current = lax.dynamic_slice_in_dim(summed, offset, BLOCK_ROWS, 1)
        summed = lax.dynamic_update_slice_in_dim(summed, current + partial_value, offset, 1)
        return summed, None

    start = jnp.zeros((CHANNELS, NODES // TILE_SIZE, TILE_SIZE), jnp.float32)
    device_ids = jnp.arange(device_count).astype(jnp.int32)
    summed, _ = lax.scan(one_device, start, (slot_rows, slot_cols, slot_live, slot_data, device_ids))
    return summed.reshape(CHANNELS, NODES).astype(jnp.bfloat16)


def reference(features, tile_rows, tile_cols, tile_count, tile_data):
    first = apply_operator(features, tile_rows, tile_cols, tile_count, tile_data)
    second = apply_operator(first, tile_rows, tile_cols, tile_count, tile_data)
    coef_zero, coef_one, coef_two = coefficients()
    base = features.astype(jnp.float32)
    first_wide = first.astype(jnp.float32)
    second_wide = second.astype(jnp.float32)
    filtered = (coef_zero[:, None, None] * base[None] + coef_one[:, None, None] * first_wide[None]
                + coef_two[:, None, None] * (2.0 * second_wide - base)[None])
    return filtered.reshape(SCALES * CHANNELS, NODES).astype(jnp.bfloat16)
```

```python
import functools

import jax
import jax.numpy as jnp
from jax import lax
from jax.experimental import pallas as pl
from jax.experimental.pallas import tpu as pltpu
from jax.sharding import PartitionSpec as P

SCALES = 8
TILE_SIZE = 128
MESH = pl.DeviceIdType.MESH
VMEM = pltpu.VMEM


def bessel_pair(times):
    halved = times / 2.0
    square = halved * halved
    term_zero = jnp.ones_like(times)
    term_one = halved
    sum_zero = term_zero
    sum_one = term_one
    for degree in range(1, 24):
        term_zero = term_zero * square / float(degree * degree)
        term_one = term_one * square / float(degree * (degree + 1))
        sum_zero = sum_zero + term_zero
        sum_one = sum_one + term_one
    damping = jnp.exp(-times)
    return (damping * sum_zero, damping * sum_one)


def coefficients():
    times = 0.25 * 2.0 ** (jnp.arange(SCALES).astype(jnp.float32) / 2.0)
    bessel_zero, bessel_one = bessel_pair(times)
    return (bessel_zero, -2.0 * bessel_one, 2.0 * (bessel_zero - 2.0 * bessel_one / times))


def gather_kernel(count, pieces, field_ref, panel_ref, own_sem, send_sem, recv_sem):
    me = lax.axis_index("row")
    barrier = pltpu.get_barrier_semaphore()
    has_right, has_left = me < count - 1, me > 0

    @pl.when(has_right)
    def _():
        pl.semaphore_signal(barrier, inc=1, device_id={"row": me + 1}, device_id_type=MESH)

    @pl.when(has_left)
    def _():
        pl.semaphore_signal(barrier, inc=1, device_id={"row": me - 1}, device_id_type=MESH)

    own = pltpu.make_async_copy(field_ref, panel_ref.at[me], own_sem)
    own.start()

    inner = jnp.logical_and(has_right, has_left)

    @pl.when(inner)
    def _():
        pl.semaphore_wait(barrier, 2)

    @pl.when(jnp.logical_not(inner))
    def _():
        pl.semaphore_wait(barrier, 1)

    depth = field_ref.shape[0] // pieces

    def transfer(way, step, piece, chunk, source=None):
        rows = pl.ds(piece * depth, depth)
        place = panel_ref.at[chunk, rows]
        return pltpu.make_async_remote_copy(
            src_ref=place if source is None else source.at[rows],
            dst_ref=place,
            send_sem=send_sem.at[way, step, piece],
            recv_sem=recv_sem.at[way, step, piece],
            device_id={"row": me + (1 if way == 0 else -1)},
            device_id_type=MESH,
        )

    for piece in range(pieces):
        for way, can in ((0, has_right), (1, has_left)):
            @pl.when(can)
            def _():
                transfer(way, 0, piece, me, field_ref).start()

    for step in range(1, count):
        for piece in range(pieces):
            for way in range(2):
                arrived = me - step if way == 0 else me + step
                inside = arrived >= 0 if way == 0 else arrived < count
                onward = has_right if way == 0 else has_left

                @pl.when(inside)
                def _():
                    transfer(way, step - 1, piece, arrived).wait_recv()

                if step < count - 1:
                    @pl.when(jnp.logical_and(inside, onward))
                    def _():
                        transfer(way, step, piece, arrived).start()

    own.wait()
    for step in range(count - 1):
        for piece in range(pieces):
            for way in range(2):
                sent = me - step if way == 0 else me + step
                inside = sent >= 0 if way == 0 else sent < count
                onward = has_right if way == 0 else has_left

                @pl.when(jnp.logical_and(inside, onward))
                def _():
                    transfer(way, step, piece, sent).wait_send()


def gather(field, count):
    channels, nodes = field.shape
    pieces = 2
    return pl.pallas_call(
        functools.partial(gather_kernel, count, pieces),
        out_shape=jax.ShapeDtypeStruct((count, channels, nodes), field.dtype),
        in_specs=[pl.BlockSpec(memory_space=VMEM)],
        out_specs=pl.BlockSpec(memory_space=VMEM),
        scratch_shapes=[
            pltpu.SemaphoreType.DMA,
            pltpu.SemaphoreType.DMA((2, count, pieces)),
            pltpu.SemaphoreType.DMA((2, count, pieces)),
        ],
        compiler_params=pltpu.CompilerParams(
            collective_id=0, has_side_effects=True, vmem_limit_bytes=40 * 2**20
        ),
        name="gather",
    )(field)


def bit_orders(count):
    bits = [1 << place for place in range(count.bit_length() - 1)]
    return (bits, bits[:1] + bits[:0:-1])


def scatter_kernel(count, partial_ref, owned_ref, arrived_ref, send_sem, recv_sem):
    me = lax.axis_index("col")
    barrier = pltpu.get_barrier_semaphore()
    orders = bit_orders(count)
    stages = len(orders[0])
    depth = partial_ref.shape[1] // 2

    def side(bit):
        return lax.rem(me // bit, 2)

    def partner(bit):
        return me + bit - 2 * bit * side(bit)

    for bit in orders[0]:
        pl.semaphore_signal(
            barrier, inc=1, device_id={"col": partner(bit)}, device_id_type=MESH
        )
    pl.semaphore_wait(barrier, stages)

    def slot_of(stage, index):
        return (1 << (stages - 1 - stage)) - 1 + index

    def first_block(half, index, away):
        order = orders[half]
        dest = order[0] * (1 - side(order[0]) if away else side(order[0]))
        for place, bit in enumerate(order[1:]):
            differs = (index >> (stages - 2 - place)) & 1
            dest = dest + bit * (1 - side(bit) if differs else side(bit))
        return partial_ref.at[dest, pl.ds(half * depth, depth)]

    def transfer(half, stage, index):
        slot = slot_of(stage, index)
        if stage == 0:
            source = first_block(half, index, True)
        else:
            source = arrived_ref.at[half, slot_of(stage - 1, index + (1 << (stages - 1 - stage)))]
        return pltpu.make_async_remote_copy(
            src_ref=source,
            dst_ref=arrived_ref.at[half, slot],
            send_sem=send_sem.at[half, slot],
            recv_sem=recv_sem.at[half, slot],
            device_id={"col": partner(orders[half][stage])},
            device_id_type=MESH,
        )

    for index in reversed(range(1 << (stages - 1))):
        for half in range(2):
            transfer(half, 0, index).start()

    for stage in range(stages):
        onward = (1 << (stages - 1 - stage)) // 2
        for index in reversed(range(1 << (stages - 1 - stage))):
            for half in range(2):
                transfer(half, stage, index).wait_recv()
                slot = slot_of(stage, index)
                if stage == 0:
                    mine = first_block(half, index, False)[...]
                else:
                    mine = arrived_ref[half, slot_of(stage - 1, index)]
                total = mine + arrived_ref[half, slot]
                if stage == stages - 1:
                    owned_ref[half * depth : (half + 1) * depth] = total
                else:
                    arrived_ref[half, slot] = total
                    if index >= onward:
                        transfer(half, stage + 1, index - onward).start()

    for stage in range(stages):
        for index in range(1 << (stages - 1 - stage)):
            for half in range(2):
                transfer(half, stage, index).wait_send()


def scatter(partial_value):
    count, channels, nodes = partial_value.shape
    return pl.pallas_call(
        functools.partial(scatter_kernel, count),
        out_shape=jax.ShapeDtypeStruct((channels, nodes), partial_value.dtype),
        in_specs=[pl.BlockSpec(memory_space=VMEM)],
        out_specs=pl.BlockSpec(memory_space=VMEM),
        scratch_shapes=[
            pltpu.VMEM((2, count - 1, channels // 2, nodes), partial_value.dtype),
            pltpu.SemaphoreType.DMA((2, count - 1)),
            pltpu.SemaphoreType.DMA((2, count - 1)),
        ],
        compiler_params=pltpu.CompilerParams(
            collective_id=1, has_side_effects=True, vmem_limit_bytes=56 * 2**20
        ),
        name="scatter",
    )(partial_value)


def tile_kernel(block, group, rows_ref, cols_ref, count_ref, panel_ref, data_ref, out_ref, acc_ref):
    step = pl.program_id(0)
    row_blocks = acc_ref.shape[0] - 1
    per_block = panel_ref.shape[2] // TILE_SIZE
    unroll = 8

    @pl.when(step == 0)
    def _():
        def clear(start, carry):
            for offset in range(unroll):
                acc_ref[start * unroll + offset] = jnp.zeros(acc_ref.shape[1:], jnp.float32)
            return carry

        lax.fori_loop(0, row_blocks // unroll, clear, 0)

    live = count_ref[0]

    def one_group(index, carry):
        start = step * block + index * group
        products = []
        for offset in range(group):
            col = cols_ref[start + offset]
            lanes = pl.ds(pl.multiple_of(lax.rem(col, per_block) * TILE_SIZE, TILE_SIZE), TILE_SIZE)
            products.append(
                lax.dot_general(
                    panel_ref[col // per_block, :, lanes],
                    data_ref[index * group + offset],
                    (((1,), (1,)), ((), ())),
                    preferred_element_type=jnp.float32,
                )
            )
        for offset in range(group):
            slot = start + offset
            row = jnp.where(slot < live, rows_ref[slot], row_blocks)
            acc_ref[row] += products[offset]
        return carry

    groups = jnp.clip((live - step * block + group - 1) // group, 0, block // group)
    lax.fori_loop(0, groups, one_group, 0)

    @pl.when(step == pl.num_programs(0) - 1)
    def _():
        per_dest = out_ref.shape[2] // TILE_SIZE

        def finish(dest, carry):
            for offset in range(per_dest):
                out_ref[dest, :, offset * TILE_SIZE : (offset + 1) * TILE_SIZE] = acc_ref[
                    dest * per_dest + offset
                ].astype(out_ref.dtype)
            return carry

        lax.fori_loop(0, out_ref.shape[0], finish, 0)


def tile_products(panel, slot_rows, slot_cols, live_count, slot_data, col_size):
    count, channels, nodes = panel.shape
    slots = slot_rows.shape[0]
    block = min(64, slots)
    group = min(8, block)
    row_blocks = col_size * nodes // TILE_SIZE
    return pl.pallas_call(
        functools.partial(tile_kernel, block, group),
        out_shape=jax.ShapeDtypeStruct((col_size, channels, nodes), panel.dtype),
        grid_spec=pltpu.PrefetchScalarGridSpec(
            num_scalar_prefetch=3,
            grid=(slots // block,),
            in_specs=[
                pl.BlockSpec(panel.shape, lambda i, *_: (0, 0, 0)),
                pl.BlockSpec((block, TILE_SIZE, TILE_SIZE), lambda i, *_: (i, 0, 0)),
            ],
            out_specs=pl.BlockSpec((col_size, channels, nodes), lambda i, *_: (0, 0, 0)),
            scratch_shapes=[pltpu.VMEM((row_blocks + 1, channels, TILE_SIZE), jnp.float32)],
        ),
        compiler_params=pltpu.CompilerParams(
            dimension_semantics=("arbitrary",), vmem_limit_bytes=56 * 2**20
        ),
        name="tiles",
    )(slot_rows, slot_cols, live_count, panel, slot_data)


def shards(features, tile_rows, tile_cols, tile_count, tile_data):
    row_size, col_size = lax.axis_size("row"), lax.axis_size("col")
    node_count = features.shape[1]
    slot_rows = tile_rows.reshape(-1)
    slot_cols = tile_cols.reshape(-1)
    slot_data = tile_data.reshape(-1, TILE_SIZE, TILE_SIZE)
    live_count = tile_count.reshape(-1)

    def apply_operator(field):
        panel = gather(field, row_size)
        partial_value = tile_products(
            panel, slot_rows, slot_cols, live_count, slot_data, col_size
        )
        return scatter(partial_value)

    first = apply_operator(features)
    second = apply_operator(first)
    coef_zero, coef_one, coef_two = coefficients()
    base = features.astype(jnp.float32)
    first_wide = first.astype(jnp.float32)
    second_wide = second.astype(jnp.float32)
    filtered = (
        coef_zero[:, None, None] * base[None]
        + coef_one[:, None, None] * first_wide[None]
        + coef_two[:, None, None] * (2.0 * second_wide - base)[None]
    )
    return filtered.reshape(-1, node_count).astype(jnp.bfloat16)


def solution(mesh):
    return jax.shard_map(
        shards,
        mesh=mesh,
        in_specs=(
            P(None, ("row", "col")),
            P("row", "col", None),
            P("row", "col", None),
            P("row", "col"),
            P("row", "col", None, None, None),
        ),
        out_specs=P(None, ("row", "col")),
        check_vma=False,
    )
```

```python
import functools

import jax
import jax.numpy as jnp
from jax import lax
from jax.experimental import pallas as pl
from jax.experimental.pallas import tpu as pltpu
from jax.sharding import PartitionSpec as P

SCALES = 8
TILE_SIZE = 128
MESH = pl.DeviceIdType.MESH
VMEM = pltpu.VMEM


def bessel_pair(times):
    halved = times / 2.0
    square = halved * halved
    term_zero = jnp.ones_like(times)
    term_one = halved
    sum_zero = term_zero
    sum_one = term_one
    for degree in range(1, 24):
        term_zero = term_zero * square / float(degree * degree)
        term_one = term_one * square / float(degree * (degree + 1))
        sum_zero = sum_zero + term_zero
        sum_one = sum_one + term_one
    damping = jnp.exp(-times)
    return (damping * sum_zero, damping * sum_one)


def coefficients():
    times = 0.25 * 2.0 ** (jnp.arange(SCALES).astype(jnp.float32) / 2.0)
    bessel_zero, bessel_one = bessel_pair(times)
    return (bessel_zero, -2.0 * bessel_one, 2.0 * (bessel_zero - 2.0 * bessel_one / times))


def bit_orders(count):
    bits = [1 << place for place in range(count.bit_length() - 1)]
    return (bits, bits[:1] + bits[:0:-1])


def gather_phases(count, pieces, field_ref, panel_ref, own_sem, send_sem, recv_sem):
    me = lax.axis_index("row")
    has_right, has_left = me < count - 1, me > 0
    depth = field_ref.shape[0] // pieces
    own = pltpu.make_async_copy(field_ref, panel_ref.at[me], own_sem)

    def transfer(way, step, piece, chunk, source=None):
        rows = pl.ds(piece * depth, depth)
        place = panel_ref.at[chunk, rows]
        return pltpu.make_async_remote_copy(
            src_ref=place if source is None else source.at[rows],
            dst_ref=place,
            send_sem=send_sem.at[way, step, piece],
            recv_sem=recv_sem.at[way, step, piece],
            device_id={"row": me + (1 if way == 0 else -1)},
            device_id_type=MESH,
        )

    def first():
        own.start()
        for piece in range(pieces):
            for way, can in ((0, has_right), (1, has_left)):
                @pl.when(can)
                def _():
                    transfer(way, 0, piece, me, field_ref).start()

    def forward(step):
        for piece in range(pieces):
            for way in range(2):
                arrived = me - step if way == 0 else me + step
                inside = arrived >= 0 if way == 0 else arrived < count
                onward = has_right if way == 0 else has_left

                @pl.when(inside)
                def _():
                    transfer(way, step - 1, piece, arrived).wait_recv()

                if step < count - 1:
                    @pl.when(jnp.logical_and(inside, onward))
                    def _():
                        transfer(way, step, piece, arrived).start()

    def last():
        own.wait()
        for step in range(count - 1):
            for piece in range(pieces):
                for way in range(2):
                    sent = me - step if way == 0 else me + step
                    inside = sent >= 0 if way == 0 else sent < count
                    onward = has_right if way == 0 else has_left

                    @pl.when(jnp.logical_and(inside, onward))
                    def _():
                        transfer(way, step, piece, sent).wait_send()

    middle = [functools.partial(forward, step) for step in range(1, count)]
    return first, middle, last


def scatter_phases(count, partial_ref, owned_ref, arrived_ref, send_sem, recv_sem):
    me = lax.axis_index("col")
    orders = bit_orders(count)
    stages = len(orders[0])
    depth = partial_ref.shape[1] // 2

    def side(bit):
        return lax.rem(me // bit, 2)

    def slot_of(stage, index):
        return (1 << (stages - 1 - stage)) - 1 + index

    def first_block(half, index, away):
        order = orders[half]
        dest = order[0] * (1 - side(order[0]) if away else side(order[0]))
        for place, bit in enumerate(order[1:]):
            differs = (index >> (stages - 2 - place)) & 1
            dest = dest + bit * (1 - side(bit) if differs else side(bit))
        return partial_ref.at[dest, pl.ds(half * depth, depth)]

    def transfer(half, stage, index):
        slot = slot_of(stage, index)
        if stage == 0:
            source = first_block(half, index, True)
        else:
            source = arrived_ref.at[half, slot_of(stage - 1, index + (1 << (stages - 1 - stage)))]
        bit = orders[half][stage]
        return pltpu.make_async_remote_copy(
            src_ref=source,
            dst_ref=arrived_ref.at[half, slot],
            send_sem=send_sem.at[half, slot],
            recv_sem=recv_sem.at[half, slot],
            device_id={"col": me + bit - 2 * bit * side(bit)},
            device_id_type=MESH,
        )

    def first():
        for index in reversed(range(1 << (stages - 1))):
            for half in range(2):
                transfer(half, 0, index).start()

    def merge(stage):
        onward = (1 << (stages - 1 - stage)) // 2
        for index in reversed(range(1 << (stages - 1 - stage))):
            for half in range(2):
                transfer(half, stage, index).wait_recv()
                slot = slot_of(stage, index)
                if stage == 0:
                    mine = first_block(half, index, False)[...]
                else:
                    mine = arrived_ref[half, slot_of(stage - 1, index)]
                total = mine + arrived_ref[half, slot]
                if stage == stages - 1:
                    owned_ref[half * depth : (half + 1) * depth] = total
                else:
                    arrived_ref[half, slot] = total
                    if index >= onward:
                        transfer(half, stage + 1, index - onward).start()

    def last():
        for stage in range(stages):
            for index in range(1 << (stages - 1 - stage)):
                for half in range(2):
                    transfer(half, stage, index).wait_send()

    middle = [functools.partial(merge, stage) for stage in range(stages)]
    return first, middle, last


def enter(row_count, col_count):
    barrier = pltpu.get_barrier_semaphore()
    peers = 0
    if col_count:
        me = lax.axis_index("col")
        for bit in bit_orders(col_count)[0]:
            other = me + bit - 2 * bit * lax.rem(me // bit, 2)
            pl.semaphore_signal(barrier, inc=1, device_id={"col": other}, device_id_type=MESH)
            peers += 1
    if not row_count:
        pl.semaphore_wait(barrier, peers)
        return
    me = lax.axis_index("row")
    has_right, has_left = me < row_count - 1, me > 0

    @pl.when(has_right)
    def _():
        pl.semaphore_signal(barrier, inc=1, device_id={"row": me + 1}, device_id_type=MESH)

    @pl.when(has_left)
    def _():
        pl.semaphore_signal(barrier, inc=1, device_id={"row": me - 1}, device_id_type=MESH)

    inner = jnp.logical_and(has_right, has_left)

    @pl.when(inner)
    def _():
        pl.semaphore_wait(barrier, peers + 2)

    @pl.when(jnp.logical_not(inner))
    def _():
        pl.semaphore_wait(barrier, peers + 1)


def exchange_kernel(row_count, col_count, pieces, *refs):
    refs = list(refs)
    inputs = [refs.pop(0) for _ in range(bool(row_count) + bool(col_count))]
    outputs = [refs.pop(0) for _ in inputs]
    enter(row_count, col_count)
    pair = []
    if row_count:
        pair.append(gather_phases(row_count, pieces, inputs[0], outputs[0], *refs[:3]))
        refs = refs[3:]
    if col_count:
        pair.append(scatter_phases(col_count, inputs[-1], outputs[-1], *refs))
    for first, _, _ in pair:
        first()
    middles = [list(middle) for _, middle, _ in pair][::-1]
    while any(middles):
        for middle in middles:
            if middle:
                middle.pop(0)()
    for _, _, last in pair:
        last()


def exchange(row_count, field, col_count, partial_value):
    pieces = 2
    operands, results, scratch = [], [], []
    if field is not None:
        channels, nodes = field.shape
        operands.append(field)
        results.append(jax.ShapeDtypeStruct((row_count, channels, nodes), field.dtype))
        scratch += [
            pltpu.SemaphoreType.DMA,
            pltpu.SemaphoreType.DMA((2, row_count, pieces)),
            pltpu.SemaphoreType.DMA((2, row_count, pieces)),
        ]
    if partial_value is not None:
        channels, nodes = partial_value.shape[1:]
        operands.append(partial_value)
        results.append(jax.ShapeDtypeStruct((channels, nodes), partial_value.dtype))
        scratch += [
            pltpu.VMEM((2, col_count - 1, channels // 2, nodes), partial_value.dtype),
            pltpu.SemaphoreType.DMA((2, col_count - 1)),
            pltpu.SemaphoreType.DMA((2, col_count - 1)),
        ]
    return pl.pallas_call(
        functools.partial(
            exchange_kernel,
            0 if field is None else row_count,
            0 if partial_value is None else col_count,
            pieces,
        ),
        out_shape=results,
        in_specs=[pl.BlockSpec(memory_space=VMEM)] * len(operands),
        out_specs=[pl.BlockSpec(memory_space=VMEM)] * len(results),
        scratch_shapes=scratch,
        compiler_params=pltpu.CompilerParams(
            collective_id=(field is not None) + 2 * (partial_value is not None),
            has_side_effects=True,
            vmem_limit_bytes=48 * 2**20,
        ),
        name="exchange",
    )(*operands)


def tile_kernel(block, group, rows_ref, cols_ref, count_ref, panel_ref, data_ref, out_ref, acc_ref):
    step = pl.program_id(0)
    row_blocks = acc_ref.shape[0] - 1
    per_block = panel_ref.shape[2] // TILE_SIZE
    unroll = 8

    @pl.when(step == 0)
    def _():
        def clear(start, carry):
            for offset in range(unroll):
                acc_ref[start * unroll + offset] = jnp.zeros(acc_ref.shape[1:], jnp.float32)
            return carry

        lax.fori_loop(0, row_blocks // unroll, clear, 0)

    live = count_ref[0]

    def one_group(index, carry):
        start = step * block + index * group
        products = []
        for offset in range(group):
            col = cols_ref[start + offset]
            lanes = pl.ds(pl.multiple_of(lax.rem(col, per_block) * TILE_SIZE, TILE_SIZE), TILE_SIZE)
            products.append(
                lax.dot_general(
                    panel_ref[col // per_block, :, lanes],
                    data_ref[index * group + offset],
                    (((1,), (1,)), ((), ())),
                    preferred_element_type=jnp.float32,
                )
            )
        for offset in range(group):
            slot = start + offset
            row = jnp.where(slot < live, rows_ref[slot], row_blocks)
            acc_ref[row] += products[offset]
        return carry

    groups = jnp.clip((live - step * block + group - 1) // group, 0, block // group)
    lax.fori_loop(0, groups, one_group, 0)

    @pl.when(step == pl.num_programs(0) - 1)
    def _():
        per_dest = out_ref.shape[2] // TILE_SIZE

        def finish(dest, carry):
            for offset in range(per_dest):
                out_ref[dest, :, offset * TILE_SIZE : (offset + 1) * TILE_SIZE] = acc_ref[
                    dest * per_dest + offset
                ].astype(out_ref.dtype)
            return carry

        lax.fori_loop(0, out_ref.shape[0], finish, 0)


def tile_products(panel, slot_rows, slot_cols, live_count, slot_data, col_size):
    count, channels, nodes = panel.shape
    slots = slot_rows.shape[0]
    block = min(64, slots)
    group = min(8, block)
    row_blocks = col_size * nodes // TILE_SIZE
    return pl.pallas_call(
        functools.partial(tile_kernel, block, group),
        out_shape=jax.ShapeDtypeStruct((col_size, channels, nodes), panel.dtype),
        grid_spec=pltpu.PrefetchScalarGridSpec(
            num_scalar_prefetch=3,
            grid=(slots // block,),
            in_specs=[
                pl.BlockSpec(panel.shape, lambda i, *_: (0, 0, 0)),
                pl.BlockSpec((block, TILE_SIZE, TILE_SIZE), lambda i, *_: (i, 0, 0)),
            ],
            out_specs=pl.BlockSpec((col_size, channels, nodes), lambda i, *_: (0, 0, 0)),
            scratch_shapes=[pltpu.VMEM((row_blocks + 1, channels, TILE_SIZE), jnp.float32)],
        ),
        compiler_params=pltpu.CompilerParams(
            dimension_semantics=("arbitrary",), vmem_limit_bytes=56 * 2**20
        ),
        name="tiles",
    )(slot_rows, slot_cols, live_count, panel, slot_data)


def shards(features, tile_rows, tile_cols, tile_count, tile_data):
    row_size, col_size = lax.axis_size("row"), lax.axis_size("col")
    node_count = features.shape[1]
    slot_rows = tile_rows.reshape(-1)
    slot_cols = tile_cols.reshape(-1)
    slot_data = tile_data.reshape(-1, TILE_SIZE, TILE_SIZE)
    live_count = tile_count.reshape(-1)

    middle = features.shape[0] // 2

    def partial_of(panel):
        return tile_products(panel, slot_rows, slot_cols, live_count, slot_data, col_size)

    def both(field, partial_value):
        return exchange(row_size, field, col_size, partial_value)

    (panel,) = both(features[:middle], None)
    partial_value = partial_of(panel)
    panel, first_low = both(features[middle:], partial_value)
    partial_value = partial_of(panel)
    panel, first_high = both(first_low, partial_value)
    partial_value = partial_of(panel)
    panel, second_low = both(first_high, partial_value)
    partial_value = partial_of(panel)
    (second_high,) = both(None, partial_value)
    first = jnp.concatenate([first_low, first_high], axis=0)
    second = jnp.concatenate([second_low, second_high], axis=0)
    coef_zero, coef_one, coef_two = coefficients()
    base = features.astype(jnp.float32)
    first_wide = first.astype(jnp.float32)
    second_wide = second.astype(jnp.float32)
    filtered = (
        coef_zero[:, None, None] * base[None]
        + coef_one[:, None, None] * first_wide[None]
        + coef_two[:, None, None] * (2.0 * second_wide - base)[None]
    )
    return filtered.reshape(-1, node_count).astype(jnp.bfloat16)


def solution(mesh):
    return jax.shard_map(
        shards,
        mesh=mesh,
        in_specs=(
            P(None, ("row", "col")),
            P("row", "col", None),
            P("row", "col", None),
            P("row", "col"),
            P("row", "col", None, None, None),
        ),
        out_specs=P(None, ("row", "col")),
        check_vma=False,
    )
```

```python
import functools

import jax
import jax.numpy as jnp
from jax import lax
from jax.experimental import pallas as pl
from jax.experimental.pallas import tpu as pltpu
from jax.sharding import PartitionSpec as P

SCALES = 8
TILE_SIZE = 128
MESH = pl.DeviceIdType.MESH
VMEM = pltpu.VMEM


def bessel_pair(times):
    halved = times / 2.0
    square = halved * halved
    term_zero = jnp.ones_like(times)
    term_one = halved
    sum_zero = term_zero
    sum_one = term_one
    for degree in range(1, 24):
        term_zero = term_zero * square / float(degree * degree)
        term_one = term_one * square / float(degree * (degree + 1))
        sum_zero = sum_zero + term_zero
        sum_one = sum_one + term_one
    damping = jnp.exp(-times)
    return (damping * sum_zero, damping * sum_one)


def coefficients():
    times = 0.25 * 2.0 ** (jnp.arange(SCALES).astype(jnp.float32) / 2.0)
    bessel_zero, bessel_one = bessel_pair(times)
    return (bessel_zero, -2.0 * bessel_one, 2.0 * (bessel_zero - 2.0 * bessel_one / times))


def gather_kernel(count, pieces, field_ref, panel_ref, own_sem, send_sem, recv_sem):
    me = lax.axis_index("row")
    barrier = pltpu.get_barrier_semaphore()
    has_right, has_left = me < count - 1, me > 0

    @pl.when(has_right)
    def _():
        pl.semaphore_signal(barrier, inc=1, device_id={"row": me + 1}, device_id_type=MESH)

    @pl.when(has_left)
    def _():
        pl.semaphore_signal(barrier, inc=1, device_id={"row": me - 1}, device_id_type=MESH)

    own = pltpu.make_async_copy(field_ref, panel_ref.at[me], own_sem)
    own.start()

    inner = jnp.logical_and(has_right, has_left)

    @pl.when(inner)
    def _():
        pl.semaphore_wait(barrier, 2)

    @pl.when(jnp.logical_not(inner))
    def _():
        pl.semaphore_wait(barrier, 1)

    depth = field_ref.shape[0] // pieces

    def transfer(way, step, piece, chunk, source=None):
        rows = pl.ds(piece * depth, depth)
        place = panel_ref.at[chunk, rows]
        return pltpu.make_async_remote_copy(
            src_ref=place if source is None else source.at[rows],
            dst_ref=place,
            send_sem=send_sem.at[way, step, piece],
            recv_sem=recv_sem.at[way, step, piece],
            device_id={"row": me + (1 if way == 0 else -1)},
            device_id_type=MESH,
        )

    for piece in range(pieces):
        for way, can in ((0, has_right), (1, has_left)):
            @pl.when(can)
            def _():
                transfer(way, 0, piece, me, field_ref).start()

    for step in range(1, count):
        for piece in range(pieces):
            for way in range(2):
                arrived = me - step if way == 0 else me + step
                inside = arrived >= 0 if way == 0 else arrived < count
                onward = has_right if way == 0 else has_left

                @pl.when(inside)
                def _():
                    transfer(way, step - 1, piece, arrived).wait_recv()

                if step < count - 1:
                    @pl.when(jnp.logical_and(inside, onward))
                    def _():
                        transfer(way, step, piece, arrived).start()

    own.wait()
    for step in range(count - 1):
        for piece in range(pieces):
            for way in range(2):
                sent = me - step if way == 0 else me + step
                inside = sent >= 0 if way == 0 else sent < count
                onward = has_right if way == 0 else has_left

                @pl.when(jnp.logical_and(inside, onward))
                def _():
                    transfer(way, step, piece, sent).wait_send()


def gather(field, count):
    channels, nodes = field.shape
    pieces = 2
    return pl.pallas_call(
        functools.partial(gather_kernel, count, pieces),
        out_shape=jax.ShapeDtypeStruct((count, channels, nodes), field.dtype),
        in_specs=[pl.BlockSpec(memory_space=VMEM)],
        out_specs=pl.BlockSpec(memory_space=VMEM),
        scratch_shapes=[
            pltpu.SemaphoreType.DMA,
            pltpu.SemaphoreType.DMA((2, count, pieces)),
            pltpu.SemaphoreType.DMA((2, count, pieces)),
        ],
        compiler_params=pltpu.CompilerParams(
            collective_id=0, has_side_effects=True, vmem_limit_bytes=40 * 2**20
        ),
        name="gather",
    )(field)


def bit_orders(count):
    bits = [1 << place for place in range(count.bit_length() - 1)]
    return (bits, bits[:1] + bits[:0:-1])


def scatter_kernel(count, partial_ref, owned_ref, arrived_ref, send_sem, recv_sem):
    me = lax.axis_index("col")
    barrier = pltpu.get_barrier_semaphore()
    orders = bit_orders(count)
    stages = len(orders[0])
    depth = partial_ref.shape[1] // 2

    def side(bit):
        return lax.rem(me // bit, 2)

    def partner(bit):
        return me + bit - 2 * bit * side(bit)

    for bit in orders[0]:
        pl.semaphore_signal(
            barrier, inc=1, device_id={"col": partner(bit)}, device_id_type=MESH
        )
    pl.semaphore_wait(barrier, stages)

    def slot_of(stage, index):
        return (1 << (stages - 1 - stage)) - 1 + index

    def first_block(half, index, away):
        order = orders[half]
        dest = order[0] * (1 - side(order[0]) if away else side(order[0]))
        for place, bit in enumerate(order[1:]):
            differs = (index >> (stages - 2 - place)) & 1
            dest = dest + bit * (1 - side(bit) if differs else side(bit))
        return partial_ref.at[dest, pl.ds(half * depth, depth)]

    def transfer(half, stage, index):
        slot = slot_of(stage, index)
        if stage == 0:
            source = first_block(half, index, True)
        else:
            source = arrived_ref.at[half, slot_of(stage - 1, index + (1 << (stages - 1 - stage)))]
        return pltpu.make_async_remote_copy(
            src_ref=source,
            dst_ref=arrived_ref.at[half, slot],
            send_sem=send_sem.at[half, slot],
            recv_sem=recv_sem.at[half, slot],
            device_id={"col": partner(orders[half][stage])},
            device_id_type=MESH,
        )

    for index in reversed(range(1 << (stages - 1))):
        for half in range(2):
            transfer(half, 0, index).start()

    for stage in range(stages):
        onward = (1 << (stages - 1 - stage)) // 2
        for index in reversed(range(1 << (stages - 1 - stage))):
            for half in range(2):
                transfer(half, stage, index).wait_recv()
                slot = slot_of(stage, index)
                if stage == 0:
                    mine = first_block(half, index, False)[...]
                else:
                    mine = arrived_ref[half, slot_of(stage - 1, index)]
                total = mine + arrived_ref[half, slot]
                if stage == stages - 1:
                    owned_ref[half * depth : (half + 1) * depth] = total
                else:
                    arrived_ref[half, slot] = total
                    if index >= onward:
                        transfer(half, stage + 1, index - onward).start()

    for stage in range(stages):
        for index in range(1 << (stages - 1 - stage)):
            for half in range(2):
                transfer(half, stage, index).wait_send()


def scatter(partial_value):
    count, channels, nodes = partial_value.shape
    return pl.pallas_call(
        functools.partial(scatter_kernel, count),
        out_shape=jax.ShapeDtypeStruct((channels, nodes), partial_value.dtype),
        in_specs=[pl.BlockSpec(memory_space=VMEM)],
        out_specs=pl.BlockSpec(memory_space=VMEM),
        scratch_shapes=[
            pltpu.VMEM((2, count - 1, channels // 2, nodes), partial_value.dtype),
            pltpu.SemaphoreType.DMA((2, count - 1)),
            pltpu.SemaphoreType.DMA((2, count - 1)),
        ],
        compiler_params=pltpu.CompilerParams(
            collective_id=1, has_side_effects=True, vmem_limit_bytes=56 * 2**20
        ),
        name="scatter",
    )(partial_value)


def tile_kernel(block, group, rows_ref, cols_ref, count_ref, panel_ref, data_ref, out_ref, acc_ref):
    step = pl.program_id(0)
    row_blocks = acc_ref.shape[0] - 1
    per_block = panel_ref.shape[2] // TILE_SIZE
    unroll = 8

    @pl.when(step == 0)
    def _():
        def clear(start, carry):
            for offset in range(unroll):
                acc_ref[start * unroll + offset] = jnp.zeros(acc_ref.shape[1:], jnp.float32)
            return carry

        lax.fori_loop(0, row_blocks // unroll, clear, 0)

    live = count_ref[0]

    def one_group(index, carry):
        start = step * block + index * group
        products = []
        for offset in range(group):
            col = cols_ref[start + offset]
            lanes = pl.ds(pl.multiple_of(lax.rem(col, per_block) * TILE_SIZE, TILE_SIZE), TILE_SIZE)
            products.append(
                lax.dot_general(
                    panel_ref[col // per_block, :, lanes],
                    data_ref[index * group + offset],
                    (((1,), (1,)), ((), ())),
                    preferred_element_type=jnp.float32,
                )
            )
        for offset in range(group):
            slot = start + offset
            row = jnp.where(slot < live, rows_ref[slot], row_blocks)
            acc_ref[row] += products[offset]
        return carry

    groups = jnp.clip((live - step * block + group - 1) // group, 0, block // group)
    lax.fori_loop(0, groups, one_group, 0)

    @pl.when(step == pl.num_programs(0) - 1)
    def _():
        per_dest = out_ref.shape[2] // TILE_SIZE

        def finish(dest, carry):
            for offset in range(per_dest):
                out_ref[dest, :, offset * TILE_SIZE : (offset + 1) * TILE_SIZE] = acc_ref[
                    dest * per_dest + offset
                ].astype(out_ref.dtype)
            return carry

        lax.fori_loop(0, out_ref.shape[0], finish, 0)


def tile_products(panel, slot_rows, slot_cols, live_count, slot_data, col_size):
    count, channels, nodes = panel.shape
    slots = slot_rows.shape[0]
    block = min(128, slots)
    group = min(16, block)
    row_blocks = col_size * nodes // TILE_SIZE
    return pl.pallas_call(
        functools.partial(tile_kernel, block, group),
        out_shape=jax.ShapeDtypeStruct((col_size, channels, nodes), panel.dtype),
        grid_spec=pltpu.PrefetchScalarGridSpec(
            num_scalar_prefetch=3,
            grid=(slots // block,),
            in_specs=[
                pl.BlockSpec(panel.shape, lambda i, *_: (0, 0, 0)),
                pl.BlockSpec((block, TILE_SIZE, TILE_SIZE), lambda i, *_: (i, 0, 0)),
            ],
            out_specs=pl.BlockSpec((col_size, channels, nodes), lambda i, *_: (0, 0, 0)),
            scratch_shapes=[pltpu.VMEM((row_blocks + 1, channels, TILE_SIZE), jnp.float32)],
        ),
        compiler_params=pltpu.CompilerParams(
            dimension_semantics=("arbitrary",), vmem_limit_bytes=56 * 2**20
        ),
        name="tiles",
    )(slot_rows, slot_cols, live_count, panel, slot_data)


def shards(features, tile_rows, tile_cols, tile_count, tile_data):
    row_size, col_size = lax.axis_size("row"), lax.axis_size("col")
    node_count = features.shape[1]
    slot_rows = tile_rows.reshape(-1)
    slot_cols = tile_cols.reshape(-1)
    slot_data = tile_data.reshape(-1, TILE_SIZE, TILE_SIZE)
    live_count = tile_count.reshape(-1)

    def apply_operator(field):
        panel = gather(field, row_size)
        partial_value = tile_products(
            panel, slot_rows, slot_cols, live_count, slot_data, col_size
        )
        return scatter(partial_value)

    first = apply_operator(features)
    second = apply_operator(first)
    coef_zero, coef_one, coef_two = coefficients()
    base = features.astype(jnp.float32)
    first_wide = first.astype(jnp.float32)
    second_wide = second.astype(jnp.float32)
    filtered = (
        coef_zero[:, None, None] * base[None]
        + coef_one[:, None, None] * first_wide[None]
        + coef_two[:, None, None] * (2.0 * second_wide - base)[None]
    )
    return filtered.reshape(-1, node_count).astype(jnp.bfloat16)


def solution(mesh):
    return jax.shard_map(
        shards,
        mesh=mesh,
        in_specs=(
            P(None, ("row", "col")),
            P("row", "col", None),
            P("row", "col", None),
            P("row", "col"),
            P("row", "col", None, None, None),
        ),
        out_specs=P(None, ("row", "col")),
        check_vma=False,
    )
```
